8 devices in a mesh: dp: 1 (over z), tp: 2 (over y), fsdp: 4 (over x, core).
Axes of the slice: x: 2, y: 2, z: 1, core: 2. Of those that a mesh axis runs over, the one named last changes fastest.
Arguments:
- x_in: bfloat16 [4, 2048, 4096], P(('dp', 'fsdp'))
- g_attn: bfloat16 [2, 4096], P(None, 'fsdp')
- w_q: bfloat16 [2, 4096, 4096], P(None, 'fsdp', 'tp')
- w_k: bfloat16 [2, 4096, 1024], P(None, 'fsdp', 'tp')
- w_v: bfloat16 [2, 4096, 1024], P(None, 'fsdp', 'tp')
- w_o: bfloat16 [2, 4096, 4096], P(None, 'tp', 'fsdp')
- g_mlp: bfloat16 [2, 4096], P(None, 'fsdp')
- w_gate: bfloat16 [2, 4096, 12288], P(None, 'fsdp', 'tp')
- w_up: bfloat16 [2, 4096, 12288], P(None, 'fsdp', 'tp')
- w_down: bfloat16 [2, 12288, 4096], P(None, 'tp', 'fsdp')
Outputs:
- output 1: bfloat16 [4, 2048, 4096], P(('dp', 'fsdp'))
- output 2: bfloat16 [2, 4, 2048, 1024], P(None, ('dp', 'fsdp'), None, 'tp')
- output 3: bfloat16 [2, 4, 2048, 1024], P(None, ('dp', 'fsdp'), None, 'tp')
All inputs are finite; a program needn't handle non-finite values.
Results may differ from the reference program's by a relative error of at most 0.02.
Values are sent between devices in bfloat16 or wider.
A program may use at most 1 GiB of HBM per device.

```python
import math
import jax
import jax.numpy as jnp
from jax import lax

BATCH_SIZE = 4
SEQ_LEN = 2048
MODEL_DIM = 4096
N_HEADS = 32
KV_HEADS = 8
HEAD_DIM = 128
FFN_DIM = 12288
N_LAYERS = 2

ROPE_THETA = 1.0e6
NORM_EPS = 1.0e-5
Q_GROUP = N_HEADS // KV_HEADS
Q_WIDTH = N_HEADS * HEAD_DIM
KV_WIDTH = KV_HEADS * HEAD_DIM
REF_BLOCK = min(SEQ_LEN, 256)


def setup_inputs(seed: int = 0, part: int = 0) -> dict:
    shared_keys = jax.random.split(jax.random.key(seed), 9)
    part_key = jax.random.fold_in(jax.random.key(seed + 1), part)
    logit_std = math.sqrt(max(math.log(SEQ_LEN / 16.0), 1.0))

    def normal_draw(key_idx, arr_shape, w_scale):
        values = jax.random.normal(shared_keys[key_idx], arr_shape, jnp.float32) * w_scale
        return values.astype(jnp.bfloat16)

    def gain_draw(key_idx):
        values = 1.0 + 0.25 * jax.random.normal(shared_keys[key_idx], (N_LAYERS, MODEL_DIM), jnp.float32)
        return values.astype(jnp.bfloat16)

    x_in = jax.random.normal(part_key, (BATCH_SIZE, SEQ_LEN, MODEL_DIM), jnp.float32)
    return {
        'x_in': x_in.astype(jnp.bfloat16),
        'g_attn': gain_draw(0),
        'w_q': normal_draw(1, (N_LAYERS, MODEL_DIM, Q_WIDTH), logit_std * MODEL_DIM ** -0.5),
        'w_k': normal_draw(2, (N_LAYERS, MODEL_DIM, KV_WIDTH), MODEL_DIM ** -0.5),
        'w_v': normal_draw(3, (N_LAYERS, MODEL_DIM, KV_WIDTH), MODEL_DIM ** -0.5),
        'w_o': normal_draw(4, (N_LAYERS, Q_WIDTH, MODEL_DIM), 2.0 * Q_WIDTH ** -0.5),
        'g_mlp': gain_draw(5),
        'w_gate': normal_draw(6, (N_LAYERS, MODEL_DIM, FFN_DIM), MODEL_DIM ** -0.5),
        'w_up': normal_draw(7, (N_LAYERS, MODEL_DIM, FFN_DIM), MODEL_DIM ** -0.5),
        'w_down': normal_draw(8, (N_LAYERS, FFN_DIM, MODEL_DIM), FFN_DIM ** -0.5),
    }


def rope_tables():
    inv_freq = ROPE_THETA ** (-2.0 * jnp.arange(HEAD_DIM // 2, dtype=jnp.float32) / HEAD_DIM)
    angles = jnp.arange(SEQ_LEN, dtype=jnp.float32)[:, None] * inv_freq[None, :]
    return jnp.cos(angles), jnp.sin(angles)


def apply_rope(t_lin, cos_t, sin_t):
    half_dim = t_lin.shape[-1] // 2
    first_half = t_lin[..., :half_dim]
    second_half = t_lin[..., half_dim:]
    cos_b = cos_t[:, None, :]
    sin_b = sin_t[:, None, :]
    return jnp.concatenate([first_half * cos_b - second_half * sin_b, second_half * cos_b + first_half * sin_b], axis=-1)


def rms_norm(x_in, gain_vec):
    x_f32 = x_in.astype(jnp.float32)
    inv_rms = lax.rsqrt(jnp.mean(x_f32 * x_f32, axis=-1, keepdims=True) + NORM_EPS)
    return (x_f32 * inv_rms * gain_vec.astype(jnp.float32)).astype(jnp.bfloat16)


def attend(q_seq, k_seq, v_seq):
    key_f = k_seq.astype(jnp.float32)
    val_f = v_seq.astype(jnp.float32)
    key_pos = jnp.arange(SEQ_LEN)
    n_blocks = SEQ_LEN // REF_BLOCK
    q_blocks = q_seq.reshape(n_blocks, REF_BLOCK, KV_HEADS, Q_GROUP, HEAD_DIM)

    def one_block(blk_args):
        q_block, blk_index = blk_args
        scores = jnp.einsum('qkgd,skd->kgqs', q_block.astype(jnp.float32), key_f) * HEAD_DIM ** -0.5
        q_pos = blk_index * REF_BLOCK + jnp.arange(REF_BLOCK)
        causal_mask = key_pos[None, :] <= q_pos[:, None]
        scores = jnp.where(causal_mask, scores, -1.0e30)
        attn_probs = jax.nn.softmax(scores, axis=-1).astype(jnp.bfloat16)
        ctx_block = jnp.einsum('kgqs,skd->qkgd', attn_probs.astype(jnp.float32), val_f)
        return ctx_block.astype(jnp.bfloat16)

    ctx_blocks = lax.map(one_block, (q_blocks, jnp.arange(n_blocks)))
    return ctx_blocks.reshape(SEQ_LEN, Q_WIDTH)


def layer_one_seq(x_seq, layer_w, cos_t, sin_t):
    g_attn, w_q, w_k, w_v, w_o, g_mlp, w_gate, w_up, w_down = layer_w
    normed = rms_norm(x_seq, g_attn)
    q_lin = jnp.dot(normed, w_q, preferred_element_type=jnp.float32).reshape(SEQ_LEN, N_HEADS, HEAD_DIM)
    k_lin = jnp.dot(normed, w_k, preferred_element_type=jnp.float32).reshape(SEQ_LEN, KV_HEADS, HEAD_DIM)
    v_val = jnp.dot(normed, w_v, preferred_element_type=jnp.float32).astype(jnp.bfloat16)
    q_rot = apply_rope(q_lin, cos_t, sin_t).astype(jnp.bfloat16)
    k_rot = apply_rope(k_lin, cos_t, sin_t).astype(jnp.bfloat16)
    context = attend(q_rot.reshape(SEQ_LEN, KV_HEADS, Q_GROUP, HEAD_DIM), k_rot, v_val.reshape(SEQ_LEN, KV_HEADS, HEAD_DIM))
    attn_out = jnp.dot(context, w_o, preferred_element_type=jnp.float32).astype(jnp.bfloat16)
    x_mid = (x_seq.astype(jnp.float32) + attn_out.astype(jnp.float32)).astype(jnp.bfloat16)
    normed_mlp = rms_norm(x_mid, g_mlp)
    gate_lin = jnp.dot(normed_mlp, w_gate, preferred_element_type=jnp.float32)
    up_lin = jnp.dot(normed_mlp, w_up, preferred_element_type=jnp.float32)
    hidden_act = (jax.nn.silu(gate_lin) * up_lin).astype(jnp.bfloat16)
    mlp_out = jnp.dot(hidden_act, w_down, preferred_element_type=jnp.float32).astype(jnp.bfloat16)
    x_next = (x_mid.astype(jnp.float32) + mlp_out.astype(jnp.float32)).astype(jnp.bfloat16)
    return x_next, k_rot.reshape(SEQ_LEN, KV_WIDTH), v_val


def reference(x_in, g_attn, w_q, w_k, w_v, w_o, g_mlp, w_gate, w_up, w_down):
    cos_t, sin_t = rope_tables()

    def layer_step(hidden, layer_w):
        def per_seq(x_seq):
            return layer_one_seq(x_seq, layer_w, cos_t, sin_t)
        x_next, k_seqs, v_seqs = lax.map(per_seq, hidden)
        return x_next, (k_seqs, v_seqs)

    x_out, caches = lax.scan(layer_step, x_in, (g_attn, w_q, w_k, w_v, w_o, g_mlp, w_gate, w_up, w_down))
    return x_out, caches[0], caches[1]
```

```python
import functools

import jax
import jax.numpy as jnp
from jax import lax
from jax.experimental import pallas as pl
from jax.experimental.pallas import tpu as pltpu
from jax.sharding import PartitionSpec as P


HEAD_DIM = 128
ROPE_THETA = 1.0e6
NORM_EPS = 1.0e-5
LOG2E = 1.4426950408889634
GU_BLOCKS = (7, 7, 6, 4)
GU_BN = 256

X, C, N, Y, K = "x", "c", "n", "y", "K"
G, Q, KV, O, GU, D, GATE, UP, DOWN = "g", "q", "kv", "o", "gu", "d", "gate", "up", "down"
I0, I1, I2, I3 = range(4)
FIRST, QKV, ATTN, OA, OB, ADDO, DA, DC, ADDM, LAST = "first", "qkv", "attn", "oa", "ob", "addo", "da", "dc", "addm", "last"

PLAN = (
    (X, Q, I0), (N, Q, I0), (X, G), (N, G), (X, KV, I0), (N, KV, I0), (X, O, I0), (C, G), (X, GU, I0, I0),
    (X, GU, I0, I1), (N, O),
    (K, FIRST, I0), (K, FIRST, I1),
    (C, Q, I0), (C, KV, I0), (X, GU, I0, I2),
    (K, QKV, I0, I0), (K, ATTN, I0, I0),
    (C, O, I0), (X, GU, I0, I3), (N, GATE), (N, UP),
    (K, OA, I0, I0), (Y, OA, I0, I0), (K, OB, I0, I0), (Y, OB, I0, I0), (K, QKV, I0, I1), (K, ATTN, I0, I1), (K, OA, I0, I1),
    (Y, OA, I0, I1), (K, OB, I0, I1), (Y, OB, I0, I1),
    (C, GU, I0, I0), (X, D, I0, I0), (N, DOWN),
    (K, ADDO, I0, I0), (K, GU, I0, I0, I0),
    (C, GU, I0, I1), (X, D, I0, I1),
    (K, GU, I0, I1, I0), (K, ADDO, I0, I1), (K, GU, I0, I0, I1),
    (C, GU, I0, I2), (X, Q, I1), (X, KV, I1),
    (K, GU, I0, I1, I1), (K, GU, I0, I2, I0),
    (C, GU, I0, I3), (X, O, I1), (N, Q, I1), (N, KV, I1),
    (K, GU, I0, I2, I1), (K, GU, I0, I3, I0), (K, DA, I0, I0), (Y, DA, I0, I0), (K, DC, I0, I0), (Y, DC, I0, I0),
    (K, GU, I0, I3, I1),
    (K, DA, I0, I1), (Y, DA, I0, I1),
    (C, D, I0, I0), (X, GU, I1, I0),
    (K, DC, I0, I1), (Y, DC, I0, I1), (K, D, I0, I0, I0), (Y, D, I0, I0, I0),
    (C, D, I0, I1), (X, GU, I1, I1),
    (K, D, I1, I0, I0), (Y, D, I1, I0, I0), (K, D, I0, I0, I1), (Y, D, I0, I0, I1), (K, D, I1, I0, I1),
    (Y, D, I1, I0, I1), (K, ADDM, I0, I0),
    (C, Q, I1), (C, KV, I1), (X, GU, I1, I2),
    (K, QKV, I1, I0), (K, ATTN, I1, I0), (K, OA, I1, I0), (Y, OA, I1, I0),
    (C, O, I1), (X, GU, I1, I3),
    (K, ADDM, I0, I1), (K, OB, I1, I0), (Y, OB, I1, I0), (K, QKV, I1, I1), (K, ATTN, I1, I1), (K, OA, I1, I1),
    (Y, OA, I1, I1),
    (K, OB, I1, I1), (Y, OB, I1, I1),
    (C, GU, I1, I0), (X, D, I1, I0),
    (K, ADDO, I1, I0), (K, GU, I1, I0, I0),
    (C, GU, I1, I1), (X, D, I1, I1),
    (K, GU, I1, I1, I0), (K, ADDO, I1, I1), (K, GU, I1, I0, I1), (K, GU, I1, I1, I1),
    (C, GU, I1, I2),
    (K, GU, I1, I2, I0), (K, GU, I1, I2, I1),
    (C, GU, I1, I3),
    (K, GU, I1, I3, I0), (K, DA, I1, I0), (Y, DA, I1, I0), (K, DC, I1, I0), (Y, DC, I1, I0), (K, GU, I1, I3, I1),
    (K, DA, I1, I1),
    (Y, DA, I1, I1), (K, DC, I1, I1), (Y, DC, I1, I1),
    (C, D, I1, I0),
    (K, D, I0, I1, I0), (Y, D, I0, I1, I0), (K, D, I0, I1, I1), (Y, D, I0, I1, I1),
    (C, D, I1, I1),
    (K, D, I1, I1, I0), (Y, D, I1, I1, I0), (K, D, I1, I1, I1), (Y, D, I1, I1, I1),
    (K, LAST, I0, I0), (K, LAST, I0, I1), (K, LAST, I1, I0), (K, LAST, I1, I1), (K, LAST, I2, I0), (K, LAST, I2, I1),
    (K, LAST, I3, I0),
    (K, LAST, I3, I1),
)

VMEM_BYTES = 62 * 1024 * 1024

F32 = jnp.float32
BF16 = jnp.bfloat16
ANY = pl.BlockSpec(memory_space=pl.ANY)


def name_of(op, *idx):
    return op + "".join(map(str, idx))


def rope_tables(seq_len):
    inv_freq = ROPE_THETA ** (-2.0 * jnp.arange(HEAD_DIM // 2, dtype=F32) / HEAD_DIM)
    angles = jnp.arange(seq_len, dtype=F32)[:, None] * inv_freq[None, :]
    cos_t, sin_t = jnp.cos(angles), jnp.sin(angles)
    return jnp.concatenate([cos_t, cos_t], axis=1), jnp.concatenate([-sin_t, sin_t], axis=1)


def params(flops_grid=1):
    return pltpu.CompilerParams(dimension_semantics=("arbitrary",) * flops_grid, vmem_limit_bytes=VMEM_BYTES)


def cost(flops, nbytes, trans=0):
    return pl.CostEstimate(flops=int(flops), bytes_accessed=int(nbytes), transcendentals=int(trans))


def left_rows(a_hbm, a_ref, a_sem, tm):
    def copy(m):
        r = pl.ds(pl.multiple_of(m * tm, tm), tm)
        return pltpu.make_async_copy(a_hbm.at[r, :], a_ref.at[r, :], a_sem.at[m])

    def start():
        for m in range(a_hbm.shape[0] // tm):
            copy(m).start()

    def wait(m):
        @pl.when(pl.program_id(0) == 0)
        def _():
            copy(m).wait()

    return start, wait


def qkv_body(a_hbm, cos_ref, sin_ref, *refs, bn, n_rope, tm):
    qs, kvs = refs[:4], refs[4:8]
    o_ref, buf, sem, a_ref, a_sem = refs[8:]
    n = pl.program_id(0)
    a_start, a_wait = left_rows(a_hbm, a_ref, a_sem, tm)
    depth = qs[0].shape[0]
    n_q = qs[0].shape[1] // bn

    def copies(ws, blk, slot):
        cols = pl.ds(pl.multiple_of(blk * bn, bn), bn)
        return [pltpu.make_async_copy(w.at[:, cols], buf.at[slot, pl.ds(i * depth, depth), :], sem.at[slot])
                for i, w in enumerate(ws)]

    @pl.when(n == 0)
    def _():
        for cp in copies(qs, 0, 0):
            cp.start()
        a_start()

    @pl.when(n + 1 < n_q)
    def _():
        for cp in copies(qs, n + 1, (n + 1) % 2):
            cp.start()

    @pl.when((n + 1 >= n_q) & (n + 1 < pl.num_programs(0)))
    def _():
        for cp in copies(kvs, n + 1 - n_q, (n + 1) % 2):
            cp.start()

    slot = n % 2
    for cp in copies(qs, 0, slot):
        cp.wait()

    def rows(m, _):
        r = pl.ds(pl.multiple_of(m * tm, tm), tm)
        a_wait(m)
        acc = jnp.dot(a_ref[r, :], buf[slot], preferred_element_type=F32)

        @pl.when(n < n_rope)
        def _():
            cos_b, sin_b = cos_ref[r, :], sin_ref[r, :]
            for h in range(bn // HEAD_DIM):
                part = acc[:, h * HEAD_DIM:(h + 1) * HEAD_DIM]
                turned = pltpu.roll(part, HEAD_DIM // 2, 1)
                o_ref[r, h * HEAD_DIM:(h + 1) * HEAD_DIM] = (part * cos_b + turned * sin_b).astype(BF16)

        @pl.when(n >= n_rope)
        def _():
            o_ref[r, :] = acc.astype(BF16)

        return 0

    lax.fori_loop(0, a_ref.shape[0] // tm, rows, 0)


def qkv_call(a, cos_t, sin_t, qs, kvs, rope_cols):
    t, k = a.shape
    n_all = qs[0].shape[1] + kvs[0].shape[1]
    bn, tm = 512, 512
    return pl.pallas_call(
        functools.partial(qkv_body, bn=bn, n_rope=rope_cols // bn, tm=tm),
        out_shape=jax.ShapeDtypeStruct((t, n_all), BF16),
        grid=(n_all // bn,),
        in_specs=[ANY, pl.BlockSpec((t, HEAD_DIM), lambda n: (0, 0)),
                  pl.BlockSpec((t, HEAD_DIM), lambda n: (0, 0))] + [ANY] * 8,
        out_specs=pl.BlockSpec((t, bn), lambda n: (0, n)),
        scratch_shapes=[pltpu.VMEM((2, k, bn), BF16), pltpu.SemaphoreType.DMA((2,)),
                        pltpu.VMEM((t, k), BF16), pltpu.SemaphoreType.DMA((t // tm,))],
        compiler_params=params(),
        cost_estimate=cost(2 * t * k * n_all, 2 * (t * k + k * n_all + t * n_all)),
    )(a, cos_t, sin_t, *qs, *kvs)


def gu_body(*refs, bn, base, tm, layer, aliased):
    a_hbm, g0, u0, g1, u1, c2, c3 = refs[:7]
    o_ref, gbuf, ubuf, sem, a_ref, a_sem = refs[7 + aliased:]
    n = pl.program_id(0)
    a_start, a_wait = left_rows(a_hbm, a_ref, a_sem, tm)
    nb = pl.num_programs(0)
    depth = c2.shape[0]
    half = c2.shape[1] // 2

    def copies(blk, slot):
        own = pl.ds(pl.multiple_of(base + blk * bn, bn), bn)
        gcol = pl.ds(pl.multiple_of(blk * bn, bn), bn)
        ucol = pl.ds(pl.multiple_of(half + blk * bn, bn), bn)
        srcs = [(g0.at[layer, :, own], u0.at[layer, :, own]), (g1.at[layer, :, own], u1.at[layer, :, own]),
                (c2.at[:, gcol], c2.at[:, ucol]), (c3.at[:, gcol], c3.at[:, ucol])]
        out = []
        for i, (gs, us) in enumerate(srcs):
            rows = pl.ds(i * depth, depth)
            out.append(pltpu.make_async_copy(gs, gbuf.at[slot, rows, :], sem.at[slot]))
            out.append(pltpu.make_async_copy(us, ubuf.at[slot, rows, :], sem.at[slot]))
        return out

    @pl.when(n == 0)
    def _():
        for cp in copies(0, 0):
            cp.start()
        a_start()

    @pl.when(n + 1 < nb)
    def _():
        for cp in copies(n + 1, (n + 1) % 2):
            cp.start()

    slot = n % 2
    for cp in copies(n, slot):
        cp.wait()

    def rows(m, _):
        r = pl.ds(pl.multiple_of(m * tm, tm), tm)
        a_wait(m)
        gate = jnp.dot(a_ref[r, :], gbuf[slot], preferred_element_type=F32)
        up = jnp.dot(a_ref[r, :], ubuf[slot], preferred_element_type=F32)
        o_ref[r, :] = (gate * jax.nn.sigmoid(gate) * up).astype(BF16)
        return 0

    lax.fori_loop(0, a_ref.shape[0] // tm, rows, 0)


def gu_call(a, g_own, u_own, g_core, u_core, c2, c3, u_prev, first, layer, f_loc):
    t, k = a.shape
    width = c2.shape[1] // 2
    bn, tm = GU_BN, 512
    nb = width // bn
    aliased = u_prev is not None
    args = [a, g_own, u_own, g_core, u_core, c2, c3] + ([u_prev] if aliased else [])
    return pl.pallas_call(
        functools.partial(gu_body, bn=bn, base=first * bn, tm=tm, layer=layer, aliased=int(aliased)),
        out_shape=jax.ShapeDtypeStruct((t, f_loc), BF16),
        grid=(nb,),
        in_specs=[ANY] * len(args),
        out_specs=pl.BlockSpec((t, bn), lambda n: (0, first + n)),
        scratch_shapes=[pltpu.VMEM((2, k, bn), BF16), pltpu.VMEM((2, k, bn), BF16), pltpu.SemaphoreType.DMA((2,)),
                        pltpu.VMEM((t, k), BF16), pltpu.SemaphoreType.DMA((t // tm,))],
        input_output_aliases={7: 0} if aliased else {},
        compiler_params=params(),
        cost_estimate=cost(4 * t * k * width, 2 * (t * k + 2 * k * width + t * width)),
    )(*args)


def cols_body(*refs, plan, n_w, tm):
    ws = refs[1:1 + n_w]
    o_ref, buf, sem, a_ref, a_sem = refs[1 + n_w:]
    n = pl.program_id(0)
    a_start, a_wait = left_rows(refs[0], a_ref, a_sem, tm)
    bw = buf.shape[2]

    def src(j):
        w, layer, col = plan[j]
        ref = ws[w]
        return ref.at[:, pl.ds(col, bw)] if layer is None else ref.at[layer, :, pl.ds(col, bw)]

    @pl.when(n == 0)
    def _():
        pltpu.make_async_copy(src(0), buf.at[0], sem.at[0]).start()
        a_start()

    for j in range(1, len(plan)):
        @pl.when(n + 1 == j)
        def _(j=j):
            pltpu.make_async_copy(src(j), buf.at[j % 2], sem.at[j % 2]).start()

    slot = n % 2
    pltpu.make_async_copy(src(0), buf.at[slot], sem.at[slot]).wait()

    def rows(m, _):
        r = pl.ds(pl.multiple_of(m * tm, tm), tm)
        a_wait(m)
        o_ref[r, :] = jnp.dot(a_ref[r, :], buf[slot], preferred_element_type=F32).astype(BF16)
        return 0

    lax.fori_loop(0, a_ref.shape[0] // tm, rows, 0)


def cols_call(a, ws, plan, bw):
    t, k = a.shape
    tm = 512
    width = bw * len(plan)
    return pl.pallas_call(
        functools.partial(cols_body, plan=plan, n_w=len(ws), tm=tm),
        out_shape=jax.ShapeDtypeStruct((t, width), BF16),
        grid=(len(plan),),
        in_specs=[ANY] * (1 + len(ws)),
        out_specs=pl.BlockSpec((t, bw), lambda n: (0, n)),
        scratch_shapes=[pltpu.VMEM((2, k, bw), BF16), pltpu.SemaphoreType.DMA((2,)),
                        pltpu.VMEM((t, k), BF16), pltpu.SemaphoreType.DMA((t // tm,))],
        compiler_params=params(),
        cost_estimate=cost(2 * t * k * width, 2 * (t * k + k * width + t * width)),
    )(a, *ws)


def attn_body(q_ref, *refs, n_past, bq, scale2):
    past_k = refs[:n_past]
    k_ref = refs[n_past]
    past_v = refs[n_past + 1:2 * n_past + 1]
    v_ref = refs[2 * n_past + 1]
    o_ref = refs[2 * n_past + 2]
    nt = (((1,), (1,)), ((), ()))
    for blk in range(q_ref.shape[0] // bq):
        lo = blk * bq
        q = q_ref[lo:lo + bq, :]
        keys = [r[...] for r in past_k] + ([k_ref[:lo, :]] if lo else [])
        vals = [r[...] for r in past_v] + ([v_ref[:lo, :]] if lo else [])
        scores = [lax.dot_general(q, kk, nt, preferred_element_type=F32) for kk in keys]
        diag = lax.dot_general(q, k_ref[lo:lo + bq, :], nt, preferred_element_type=F32)
        row = lax.broadcasted_iota(jnp.int32, (bq, bq), 0)
        col = lax.broadcasted_iota(jnp.int32, (bq, bq), 1)
        scores.append(jnp.where(col <= row, diag, -1.0e30))
        vals.append(v_ref[lo:lo + bq, :])
        top = jnp.max(scores[0], axis=1, keepdims=True)
        for s in scores[1:]:
            top = jnp.maximum(top, jnp.max(s, axis=1, keepdims=True))
        probs = [jnp.exp2((s - top) * scale2) for s in scores]
        total = jnp.sum(probs[0], axis=1, keepdims=True)
        for p in probs[1:]:
            total = total + jnp.sum(p, axis=1, keepdims=True)
        inv = 1.0 / total
        ctx = None
        for p, vv in zip(probs, vals):
            part = jnp.dot((p * inv).astype(BF16), vv, preferred_element_type=F32)
            ctx = part if ctx is None else ctx + part
        o_ref[lo:lo + bq, :] = ctx.astype(BF16)


def attn_call(qkv, past, n_q, n_kv):
    t = qkv.shape[0]
    group = n_q // n_kv

    def k_spec(arr):
        return pl.BlockSpec((arr.shape[0], HEAD_DIM), lambda h: (0, n_q + h // group))

    def v_spec(arr):
        return pl.BlockSpec((arr.shape[0], HEAD_DIM), lambda h: (0, n_q + n_kv + h // group))

    arrs = list(past) + [qkv]
    seen = sum(p.shape[0] for p in past) * t + t * t // 2
    return pl.pallas_call(
        functools.partial(attn_body, n_past=len(past), bq=256, scale2=HEAD_DIM ** -0.5 * LOG2E),
        out_shape=jax.ShapeDtypeStruct((t, n_q * HEAD_DIM), BF16),
        grid=(n_q,),
        in_specs=[pl.BlockSpec((t, HEAD_DIM), lambda h: (0, h))] + [k_spec(a) for a in arrs] + [v_spec(a) for a in arrs],
        out_specs=pl.BlockSpec((t, HEAD_DIM), lambda h: (0, h)),
        compiler_params=params(),
        cost_estimate=cost(4 * 4 * n_q * seen * HEAD_DIM, 2 * 2 * t * n_q * HEAD_DIM, n_q * seen),
    )(qkv, *arrs, *arrs)


def norm_rows(x, g_row):
    xf = x.astype(F32)
    inv = lax.rsqrt(jnp.mean(xf * xf, axis=-1, keepdims=True) + NORM_EPS)
    return (xf * inv * g_row).astype(BF16)


def first_body(_, x0, x1, x2, x3, g_ref, xp_ref, h_ref):
    x = jnp.concatenate([r[...] for r in (x0, x1, x2, x3)], axis=1)
    xp_ref[...] = x
    h_ref[...] = norm_rows(x, g_ref[...])


def first_call(x, order, g, row0, t):
    d = x.shape[1]
    q = d // 4
    tb = 128
    blk = [pl.BlockSpec((tb, q), lambda r, o, i=i: (row0 // tb + r, o[i])) for i in range(4)]
    row = pl.BlockSpec((tb, d), lambda r, o: (r, 0))
    return pl.pallas_call(
        first_body,
        grid_spec=pltpu.PrefetchScalarGridSpec(
            num_scalar_prefetch=1, grid=(t // tb,),
            in_specs=blk + [pl.BlockSpec((1, d), lambda r, o: (0, 0))], out_specs=[row, row]),
        out_shape=[jax.ShapeDtypeStruct((t, d), BF16)] * 2,
        compiler_params=params(), cost_estimate=cost(10 * t * d, 6 * t * d),
    )(order, x, x, x, x, g)


def add_body(*refs, segs):
    n = len(segs)
    x_ref = refs[0]
    ps, rs = refs[1:1 + n], refs[1 + n:1 + 2 * n]
    g_ref, xo_ref, h_ref = refs[1 + 2 * n:]
    for p, r, seg in zip(ps, rs, segs):
        for src, dst, w in seg:
            a = (p[:, src:src + w].astype(F32) + r[:, src:src + w].astype(F32)).astype(BF16)
            xo_ref[:, dst:dst + w] = (x_ref[:, dst:dst + w].astype(F32) + a.astype(F32)).astype(BF16)
    h_ref[...] = norm_rows(xo_ref[...], g_ref[...])


def add_call(x, units, g):
    t, d = x.shape
    tb = 128
    row = pl.BlockSpec((tb, d), lambda r: (r, 0))
    ps, rs, segs = [u[0] for u in units], [u[1] for u in units], [u[2] for u in units]
    return pl.pallas_call(
        functools.partial(add_body, segs=segs),
        grid=(t // tb,),
        in_specs=[row] + [pl.BlockSpec((tb, a.shape[1]), lambda r: (r, 0)) for a in ps + rs]
        + [pl.BlockSpec((1, d), lambda r: (0, 0))],
        out_specs=[row, row],
        out_shape=[jax.ShapeDtypeStruct((t, d), BF16)] * 2,
        compiler_params=params(), cost_estimate=cost(12 * t * d, 10 * t * d),
    )(x, *ps, *rs, g)


def last_body(_, x_ref, p_ref, r_ref, *rest):
    o_ref = rest[-1]
    a = (p_ref[...].astype(F32) + r_ref[...].astype(F32)).astype(BF16)
    o_ref[...] = (x_ref[...].astype(F32) + a.astype(F32)).astype(BF16)


def last_call(x, unit, order, out_prev, row0, rows):
    p, r, seg = unit
    t, d = x.shape
    w = seg[0][2]
    per = d // 4 // w
    tb = 512
    dst = [s[1] // w for s in seg]
    step = (dst[1] - dst[0]) if len(dst) > 1 else 0
    assert all(dst[j] == dst[0] + j * step for j in range(len(dst)))
    base = dst[0]

    def x_map(j, i, o):
        return (i, base + j * step)

    def o_map(j, i, o):
        pb = base + j * step
        return (row0 // tb + i, o[pb // per] * per + pb % per)

    unit_spec = pl.BlockSpec((tb, w), lambda j, i, o: (i, j))
    args = [x, p, r] + ([out_prev] if out_prev is not None else [])
    return pl.pallas_call(
        last_body,
        grid_spec=pltpu.PrefetchScalarGridSpec(
            num_scalar_prefetch=1, grid=(len(seg), t // tb),
            in_specs=[pl.BlockSpec((tb, w), x_map), unit_spec, unit_spec] + [ANY] * (len(args) - 3),
            out_specs=pl.BlockSpec((tb, w), o_map)),
        out_shape=jax.ShapeDtypeStruct((rows, d), BF16),
        input_output_aliases={4: 0} if out_prev is not None else {},
        compiler_params=params(2), cost_estimate=cost(4 * t * w * len(seg), 8 * t * w * len(seg)),
    )(order, *args)


def solution(mesh):
    n_tp, n_fsdp = mesh.shape["tp"], mesh.shape["fsdp"]
    assert n_tp == 2 and n_fsdp == 4
    tok_spec = P(("dp", "fsdp"), None, None)
    gain_spec = P(None, "fsdp")
    col_spec = P(None, "fsdp", "tp")
    row_spec = P(None, "tp", "fsdp")
    cache_spec = P(None, ("dp", "fsdp"), None, "tp")
    far = [(i, i ^ 2) for i in range(4)]
    near = [(i, i ^ 1) for i in range(4)]
    swap = [(0, 1), (1, 0)]

    def device_fn(x_loc, g_attn, w_q, w_k, w_v, w_o, g_mlp, w_gate, w_up, w_down):
        _, seq, d = x_loc.shape
        n_layers = w_q.shape[0]
        qw, kw = w_q.shape[2], w_k.shape[2]
        f_loc = w_gate.shape[2]
        n_q, n_kv = qw // HEAD_DIM, kw // HEAD_DIM
        quarter = d // 4
        half_t = seq // 2
        assert sum(GU_BLOCKS) * GU_BN == f_loc
        dw = quarter // 2
        me = lax.axis_index("fsdp")
        order = jnp.stack([me, me ^ 1, me ^ 2, me ^ 3]).astype(jnp.int32)
        cos_t, sin_t = rope_tables(seq)
        x2 = x_loc.reshape(seq, d)

        def wide(l, i):
            lo, hi = sum(GU_BLOCKS[:i]) * GU_BN, sum(GU_BLOCKS[:i + 1]) * GU_BN
            return jnp.concatenate([w_gate[l][:, lo:hi], w_up[l][:, lo:hi]], axis=1)

        own = {O: w_o, GATE: w_gate, UP: w_up, DOWN: w_down, G: jnp.concatenate([g_attn, g_mlp], axis=0)}
        for l in range(n_layers):
            own[name_of(O, l)] = w_o[l]
            for i in range(len(GU_BLOCKS)):
                own[name_of(GU, l, i)] = wide(l, i)
            for i in range(2):
                own[name_of(D, l, i)] = w_down[l][:, i * dw:(i + 1) * dw]

        seg_a = [(0, 0, quarter), (quarter, quarter, quarter)]
        seg_own, seg_core = [(0, 0, quarter)], [(0, quarter, quarter)]
        seg_b = [(0, 2 * quarter, quarter), (quarter, 3 * quarter, quarter)]
        seg_d = [[(0, 2 * quarter + i * dw, dw), (dw, 3 * quarter + i * dw, dw)] for i in range(2)]

        xr, cr, nr, part, yr = {}, {}, {}, {}, {}
        hid, hn, qkv, ctx, acts = {}, {}, {}, {}, {}
        out, gains = [None], []

        def pieces(key):
            return [own[key], nr[key], xr[key], cr[key]]

        def kernel(name, dep, op, *idx):
            s, l = idx[-1], idx[-2] if op in (D, QKV, ATTN, OA, OB, ADDO, DA, DC, ADDM) else idx[0]
            if op == FIRST:
                if not gains:
                    rows = jnp.concatenate(pieces(G), axis=1).astype(F32)
                    gains.extend(rows[i:i + 1] for i in range(2 * n_layers))
                hid[s], hn[s] = first_call(dep(x2), order, gains[0], s * half_t, half_t)
                return hn[s]
            if op == QKV:
                rows = slice(s * half_t, (s + 1) * half_t)
                qkv[s] = qkv_call(dep(hn[s]), cos_t[rows], sin_t[rows], pieces(name_of(Q, l)), pieces(name_of(KV, l)),
                                  qw + kw)
                return qkv[s]
            if op == ATTN:
                ctx[s] = attn_call(dep(qkv[s]), [qkv[p] for p in range(s)], n_q, n_kv)
                return ctx[s]
            if op == OA:
                plan = [(0, l, 0), (0, l, dw), (1, l, 0), (1, l, dw)]
                part[name] = cols_call(dep(ctx[s]), [w_o, nr[O]], plan, dw)
                return part[name]
            if op in (DA, DC):
                w = w_down if op == DA else nr[DOWN]
                part[name] = cols_call(dep(acts[s]), [w], [(0, l, 0), (0, l, dw)], dw)
                return part[name]
            if op == OB:
                key = name_of(O, l)
                plan = [(0, None, 0), (0, None, dw), (1, None, 0), (1, None, dw)]
                part[name] = cols_call(dep(ctx[s]), [xr[key], cr[key]], plan, dw)
                return part[name]
            if op == D:
                key = name_of(D, l, idx[0])
                part[name] = cols_call(dep(acts[s]), [xr[key], cr[key]], [(0, None, 0), (1, None, 0)], dw)
                return part[name]
            if op == GU:
                i = idx[1]
                key = name_of(GU, l, i)
                acts[s] = gu_call(dep(hn[s]), w_gate, w_up, nr[GATE], nr[UP], xr[key], cr[key],
                                  acts[s] if i else None, sum(GU_BLOCKS[:i]), l, f_loc)
                return acts[s]
            if op == ADDO:
                tags = [name_of(w, l, s) for w in (OA, OB)]
                units = [(part[t], yr[t], g) for t, g in zip(tags, (seg_a, seg_b))]
                hid[s], hn[s] = add_call(dep(hid[s]), units, gains[n_layers + l])
                return hn[s]
            last_l = l if op == ADDM else n_layers - 1
            tags = [name_of(DA, last_l, s), name_of(DC, last_l, s), name_of(D, 0, last_l, s), name_of(D, 1, last_l, s)]
            segs = [seg_own, seg_core] + seg_d
            if op == ADDM:
                units = [(part[t], yr[t], g) for t, g in zip(tags, segs)]
                hid[s], hn[s] = add_call(dep(hid[s]), units, gains[l + 1])
                return hn[s]
            i = idx[0]
            unit = (part[tags[i]], yr[tags[i]], segs[i])
            out[0] = last_call(dep(hid[s]), unit, order, out[0], s * half_t, seq)
            return out[0]

        caches = []
        last = None
        for kind, *what in PLAN:
            name = name_of(*what)

            def dep(x):
                return x if last is None else lax.optimization_barrier((x, last))[0]

            if kind == X and what[0] == Q:
                own[name] = dep(w_q)[what[1]]
            elif kind == X and what[0] == KV:
                own[name] = jnp.concatenate([dep(w_k)[what[1]], dep(w_v)[what[1]]], axis=1)
            if kind == X:
                xr[name] = lax.ppermute(dep(own[name]), "fsdp", far)
            elif kind == C:
                cr[name] = lax.ppermute(dep(xr[name]), "fsdp", near)
            elif kind == N:
                nr[name] = lax.ppermute(own[name], "fsdp", near)
            elif kind == Y:
                yr[name] = lax.ppermute(part[name], "tp", swap)
            else:
                last = kernel(name, dep, *what)
            if kind == K and what[0] == QKV and what[-1] == 1:
                caches.append([jnp.concatenate([qkv[s][:, lo:lo + kw] for s in range(2)], axis=0)
                               for lo in (qw, qw + kw)])
        k_all, v_all = (jnp.stack([c[j] for c in caches])[:, None] for j in range(2))
        return out[0].reshape(1, seq, d), k_all, v_all

    return jax.shard_map(
        device_fn, mesh=mesh,
        in_specs=(tok_spec, gain_spec, col_spec, col_spec, col_spec, row_spec, gain_spec, col_spec, col_spec, row_spec),
        out_specs=(tok_spec, cache_spec, cache_spec), check_vma=False)
```

```python
import functools

import jax
import jax.numpy as jnp
from jax import lax
from jax.experimental import pallas as pl
from jax.experimental.pallas import tpu as pltpu
from jax.sharding import PartitionSpec as P


HEAD_DIM = 128
ROPE_THETA = 1.0e6
NORM_EPS = 1.0e-5
LOG2E = 1.4426950408889634
GU_BLOCKS = (7, 7, 5, 3, 2)
GU_BN = 256

X, C, N, Y, K = "x", "c", "n", "y", "K"
G, Q, KV, O, GU, D, GATE, UP, DOWN = "g", "q", "kv", "o", "gu", "d", "gate", "up", "down"
I0, I1, I2, I3, I4 = range(5)
FIRST, QKV, ATTN, OA, OB, ADDO = "first", "qkv", "attn", "oa", "ob", "addo"
DA, DB, DC, ADDM, LAST = "da", "db", "dc", "addm", "last"

PLAN = (
    (X, Q, I0), (N, Q, I0), (X, G), (N, G), (X, KV, I0), (N, KV, I0), (X, O, I0), (C, G), (X, GU, I0, I0), (X, GU, I0, I1),
    (N, O),
    (K, FIRST, I0), (K, FIRST, I1),
    (C, Q, I0), (C, KV, I0), (X, GU, I0, I2),
    (K, QKV, I0, I0), (K, ATTN, I0, I0),
    (C, O, I0), (X, GU, I0, I3), (X, GU, I0, I4), (N, GATE), (N, UP),
    (K, OA, I0, I0), (Y, OA, I0, I0), (K, OB, I0, I0), (Y, OB, I0, I0), (K, QKV, I0, I1), (K, ATTN, I0, I1),
    (K, OA, I0, I1), (Y, OA, I0, I1), (K, OB, I0, I1), (Y, OB, I0, I1),
    (C, GU, I0, I0), (X, D, I0, I0), (N, DOWN),
    (K, ADDO, I0, I0), (K, GU, I0, I0, I0),
    (C, GU, I0, I1), (X, D, I0, I1),
    (K, GU, I0, I1, I0), (K, ADDO, I0, I1), (K, GU, I0, I0, I1),
    (C, GU, I0, I2), (X, Q, I1), (X, KV, I1),
    (K, GU, I0, I1, I1), (K, GU, I0, I2, I0),
    (C, GU, I0, I3), (X, O, I1), (N, Q, I1), (N, KV, I1),
    (K, GU, I0, I2, I1),
    (C, GU, I0, I4), (X, GU, I1, I0),
    (K, GU, I0, I3, I0), (K, GU, I0, I4, I0), (K, DA, I0, I0), (Y, DA, I0, I0), (K, DB, I0, I0), (Y, DB, I0, I0),
    (K, DC, I0, I0), (Y, DC, I0, I0), (K, GU, I0, I3, I1), (K, GU, I0, I4, I1), (K, DA, I0, I1), (Y, DA, I0, I1),
    (K, DB, I0, I1), (Y, DB, I0, I1),
    (C, D, I0, I0), (X, GU, I1, I1),
    (K, DC, I0, I1), (Y, DC, I0, I1), (K, D, I0, I0, I0), (Y, D, I0, I0, I0),
    (C, D, I0, I1), (X, GU, I1, I2),
    (K, D, I1, I0, I0), (Y, D, I1, I0, I0), (K, D, I0, I0, I1), (Y, D, I0, I0, I1), (K, D, I1, I0, I1), (Y, D, I1, I0, I1),
    (K, ADDM, I0, I0),
    (C, Q, I1), (C, KV, I1), (X, GU, I1, I3), (X, GU, I1, I4),
    (K, QKV, I1, I0), (K, ATTN, I1, I0), (K, OA, I1, I0), (Y, OA, I1, I0),
    (C, O, I1), (X, D, I1, I0),
    (K, ADDM, I0, I1), (K, OB, I1, I0), (Y, OB, I1, I0), (K, QKV, I1, I1), (K, ATTN, I1, I1), (K, OA, I1, I1),
    (Y, OA, I1, I1), (K, OB, I1, I1), (Y, OB, I1, I1),
    (C, GU, I1, I0), (X, D, I1, I1),
    (K, ADDO, I1, I0), (K, GU, I1, I0, I0),
    (C, GU, I1, I1),
    (K, GU, I1, I1, I0), (K, ADDO, I1, I1), (K, GU, I1, I0, I1),
    (C, GU, I1, I2),
    (K, GU, I1, I1, I1), (K, GU, I1, I2, I0),
    (C, GU, I1, I3),
    (K, GU, I1, I2, I1), (K, GU, I1, I3, I0),
    (C, GU, I1, I4),
    (K, GU, I1, I4, I0), (K, DA, I1, I0), (Y, DA, I1, I0), (K, DB, I1, I0), (Y, DB, I1, I0), (K, DC, I1, I0),
    (Y, DC, I1, I0), (K, GU, I1, I3, I1), (K, GU, I1, I4, I1), (K, DA, I1, I1), (Y, DA, I1, I1), (K, DB, I1, I1),
    (Y, DB, I1, I1), (K, DC, I1, I1), (Y, DC, I1, I1),
    (C, D, I1, I0),
    (K, D, I0, I1, I0), (Y, D, I0, I1, I0), (K, D, I0, I1, I1), (Y, D, I0, I1, I1),
    (C, D, I1, I1),
    (K, D, I1, I1, I0), (Y, D, I1, I1, I0), (K, D, I1, I1, I1), (Y, D, I1, I1, I1),
    (K, LAST, I0, I0), (K, LAST, I0, I1), (K, LAST, I1, I0), (K, LAST, I1, I1), (K, LAST, I2, I0), (K, LAST, I2, I1),
    (K, LAST, I3, I0), (K, LAST, I3, I1), (K, LAST, I4, I0), (K, LAST, I4, I1),
)

VMEM_BYTES = 62 * 1024 * 1024

F32 = jnp.float32
BF16 = jnp.bfloat16
ANY = pl.BlockSpec(memory_space=pl.ANY)


def name_of(op, *idx):
    return op + "".join(map(str, idx))


def rope_tables(seq_len):
    inv_freq = ROPE_THETA ** (-2.0 * jnp.arange(HEAD_DIM // 2, dtype=F32) / HEAD_DIM)
    angles = jnp.arange(seq_len, dtype=F32)[:, None] * inv_freq[None, :]
    cos_t, sin_t = jnp.cos(angles), jnp.sin(angles)
    return jnp.concatenate([cos_t, cos_t], axis=1), jnp.concatenate([-sin_t, sin_t], axis=1)


def params(flops_grid=1):
    return pltpu.CompilerParams(dimension_semantics=("arbitrary",) * flops_grid, vmem_limit_bytes=VMEM_BYTES)


def cost(flops, nbytes, trans=0):
    return pl.CostEstimate(flops=int(flops), bytes_accessed=int(nbytes), transcendentals=int(trans))


def left_rows(a_hbm, a_ref, a_sem, tm):
    def copy(m):
        r = pl.ds(pl.multiple_of(m * tm, tm), tm)
        return pltpu.make_async_copy(a_hbm.at[r, :], a_ref.at[r, :], a_sem.at[m])

    def start():
        for m in range(a_hbm.shape[0] // tm):
            copy(m).start()

    def wait(m):
        @pl.when(pl.program_id(0) == 0)
        def _():
            copy(m).wait()

    return start, wait


def qkv_body(a_hbm, cos_ref, sin_ref, *refs, bn, n_rope, tm):
    qs, kvs = refs[:4], refs[4:8]
    o_ref, buf, sem, a_ref, a_sem = refs[8:]
    n = pl.program_id(0)
    a_start, a_wait = left_rows(a_hbm, a_ref, a_sem, tm)
    depth = qs[0].shape[0]
    n_q = qs[0].shape[1] // bn

    def copies(ws, blk, slot):
        cols = pl.ds(pl.multiple_of(blk * bn, bn), bn)
        return [pltpu.make_async_copy(w.at[:, cols], buf.at[slot, pl.ds(i * depth, depth), :], sem.at[slot])
                for i, w in enumerate(ws)]

    @pl.when(n == 0)
    def _():
        for cp in copies(qs, 0, 0):
            cp.start()
        a_start()

    @pl.when(n + 1 < n_q)
    def _():
        for cp in copies(qs, n + 1, (n + 1) % 2):
            cp.start()

    @pl.when((n + 1 >= n_q) & (n + 1 < pl.num_programs(0)))
    def _():
        for cp in copies(kvs, n + 1 - n_q, (n + 1) % 2):
            cp.start()

    slot = n % 2
    for cp in copies(qs, 0, slot):
        cp.wait()

    def rows(m, _):
        r = pl.ds(pl.multiple_of(m * tm, tm), tm)
        a_wait(m)
        acc = jnp.dot(a_ref[r, :], buf[slot], preferred_element_type=F32)

        @pl.when(n < n_rope)
        def _():
            cos_b, sin_b = cos_ref[r, :], sin_ref[r, :]
            for h in range(bn // HEAD_DIM):
                part = acc[:, h * HEAD_DIM:(h + 1) * HEAD_DIM]
                turned = pltpu.roll(part, HEAD_DIM // 2, 1)
                o_ref[r, h * HEAD_DIM:(h + 1) * HEAD_DIM] = (part * cos_b + turned * sin_b).astype(BF16)

        @pl.when(n >= n_rope)
        def _():
            o_ref[r, :] = acc.astype(BF16)

        return 0

    lax.fori_loop(0, a_ref.shape[0] // tm, rows, 0)


def qkv_call(a, cos_t, sin_t, qs, kvs, rope_cols):
    t, k = a.shape
    n_all = qs[0].shape[1] + kvs[0].shape[1]
    bn, tm = 512, 512
    return pl.pallas_call(
        functools.partial(qkv_body, bn=bn, n_rope=rope_cols // bn, tm=tm),
        out_shape=jax.ShapeDtypeStruct((t, n_all), BF16),
        grid=(n_all // bn,),
        in_specs=[ANY, pl.BlockSpec((t, HEAD_DIM), lambda n: (0, 0)),
                  pl.BlockSpec((t, HEAD_DIM), lambda n: (0, 0))] + [ANY] * 8,
        out_specs=pl.BlockSpec((t, bn), lambda n: (0, n)),
        scratch_shapes=[pltpu.VMEM((2, k, bn), BF16), pltpu.SemaphoreType.DMA((2,)),
                        pltpu.VMEM((t, k), BF16), pltpu.SemaphoreType.DMA((t // tm,))],
        compiler_params=params(),
        cost_estimate=cost(2 * t * k * n_all, 2 * (t * k + k * n_all + t * n_all)),
    )(a, cos_t, sin_t, *qs, *kvs)


def gu_body(*refs, bn, base, tm, layer, aliased):
    a_hbm, g0, u0, g1, u1, c2, c3 = refs[:7]
    o_ref, gbuf, ubuf, sem, a_ref, a_sem = refs[7 + aliased:]
    n = pl.program_id(0)
    a_start, a_wait = left_rows(a_hbm, a_ref, a_sem, tm)
    nb = pl.num_programs(0)
    depth = c2.shape[0]
    half = c2.shape[1] // 2

    def copies(blk, slot):
        own = pl.ds(pl.multiple_of(base + blk * bn, bn), bn)
        gcol = pl.ds(pl.multiple_of(blk * bn, bn), bn)
        ucol = pl.ds(pl.multiple_of(half + blk * bn, bn), bn)
        srcs = [(g0.at[layer, :, own], u0.at[layer, :, own]), (g1.at[layer, :, own], u1.at[layer, :, own]),
                (c2.at[:, gcol], c2.at[:, ucol]), (c3.at[:, gcol], c3.at[:, ucol])]
        out = []
        for i, (gs, us) in enumerate(srcs):
            rows = pl.ds(i * depth, depth)
            out.append(pltpu.make_async_copy(gs, gbuf.at[slot, rows, :], sem.at[slot]))
            out.append(pltpu.make_async_copy(us, ubuf.at[slot, rows, :], sem.at[slot]))
        return out

    @pl.when(n == 0)
    def _():
        for cp in copies(0, 0):
            cp.start()
        a_start()

    @pl.when(n + 1 < nb)
    def _():
        for cp in copies(n + 1, (n + 1) % 2):
            cp.start()

    slot = n % 2
    for cp in copies(n, slot):
        cp.wait()

    def rows(m, _):
        r = pl.ds(pl.multiple_of(m * tm, tm), tm)
        a_wait(m)
        gate = jnp.dot(a_ref[r, :], gbuf[slot], preferred_element_type=F32)
        up = jnp.dot(a_ref[r, :], ubuf[slot], preferred_element_type=F32)
        o_ref[r, :] = (gate * jax.nn.sigmoid(gate) * up).astype(BF16)
        return 0

    lax.fori_loop(0, a_ref.shape[0] // tm, rows, 0)


def gu_call(a, g_own, u_own, g_core, u_core, c2, c3, u_prev, first, layer, f_loc):
    t, k = a.shape
    width = c2.shape[1] // 2
    bn, tm = GU_BN, 512
    nb = width // bn
    aliased = u_prev is not None
    args = [a, g_own, u_own, g_core, u_core, c2, c3] + ([u_prev] if aliased else [])
    return pl.pallas_call(
        functools.partial(gu_body, bn=bn, base=first * bn, tm=tm, layer=layer, aliased=int(aliased)),
        out_shape=jax.ShapeDtypeStruct((t, f_loc), BF16),
        grid=(nb,),
        in_specs=[ANY] * len(args),
        out_specs=pl.BlockSpec((t, bn), lambda n: (0, first + n)),
        scratch_shapes=[pltpu.VMEM((2, k, bn), BF16), pltpu.VMEM((2, k, bn), BF16), pltpu.SemaphoreType.DMA((2,)),
                        pltpu.VMEM((t, k), BF16), pltpu.SemaphoreType.DMA((t // tm,))],
        input_output_aliases={7: 0} if aliased else {},
        compiler_params=params(),
        cost_estimate=cost(4 * t * k * width, 2 * (t * k + 2 * k * width + t * width)),
    )(*args)


def cols_body(*refs, plan, n_w, tm):
    ws = refs[1:1 + n_w]
    o_ref, buf, sem, a_ref, a_sem = refs[1 + n_w:]
    n = pl.program_id(0)
    a_start, a_wait = left_rows(refs[0], a_ref, a_sem, tm)
    bw = buf.shape[2]

    def src(j):
        w, layer, col = plan[j]
        ref = ws[w]
        return ref.at[:, pl.ds(col, bw)] if layer is None else ref.at[layer, :, pl.ds(col, bw)]

    @pl.when(n == 0)
    def _():
        pltpu.make_async_copy(src(0), buf.at[0], sem.at[0]).start()
        a_start()

    for j in range(1, len(plan)):
        @pl.when(n + 1 == j)
        def _(j=j):
            pltpu.make_async_copy(src(j), buf.at[j % 2], sem.at[j % 2]).start()

    slot = n % 2
    pltpu.make_async_copy(src(0), buf.at[slot], sem.at[slot]).wait()

    def rows(m, _):
        r = pl.ds(pl.multiple_of(m * tm, tm), tm)
        a_wait(m)
        o_ref[r, :] = jnp.dot(a_ref[r, :], buf[slot], preferred_element_type=F32).astype(BF16)
        return 0

    lax.fori_loop(0, a_ref.shape[0] // tm, rows, 0)


def cols_call(a, ws, plan, bw):
    t, k = a.shape
    tm = 512
    width = bw * len(plan)
    return pl.pallas_call(
        functools.partial(cols_body, plan=plan, n_w=len(ws), tm=tm),
        out_shape=jax.ShapeDtypeStruct((t, width), BF16),
        grid=(len(plan),),
        in_specs=[ANY] * (1 + len(ws)),
        out_specs=pl.BlockSpec((t, bw), lambda n: (0, n)),
        scratch_shapes=[pltpu.VMEM((2, k, bw), BF16), pltpu.SemaphoreType.DMA((2,)),
                        pltpu.VMEM((t, k), BF16), pltpu.SemaphoreType.DMA((t // tm,))],
        compiler_params=params(),
        cost_estimate=cost(2 * t * k * width, 2 * (t * k + k * width + t * width)),
    )(a, *ws)


def attn_body(q_ref, *refs, n_past, bq, scale2):
    past_k = refs[:n_past]
    k_ref = refs[n_past]
    past_v = refs[n_past + 1:2 * n_past + 1]
    v_ref = refs[2 * n_past + 1]
    o_ref = refs[2 * n_past + 2]
    nt = (((1,), (1,)), ((), ()))
    for blk in range(q_ref.shape[0] // bq):
        lo = blk * bq
        q = q_ref[lo:lo + bq, :]
        keys = [r[...] for r in past_k] + ([k_ref[:lo, :]] if lo else [])
        vals = [r[...] for r in past_v] + ([v_ref[:lo, :]] if lo else [])
        scores = [lax.dot_general(q, kk, nt, preferred_element_type=F32) for kk in keys]
        diag = lax.dot_general(q, k_ref[lo:lo + bq, :], nt, preferred_element_type=F32)
        row = lax.broadcasted_iota(jnp.int32, (bq, bq), 0)
        col = lax.broadcasted_iota(jnp.int32, (bq, bq), 1)
        scores.append(jnp.where(col <= row, diag, -1.0e30))
        vals.append(v_ref[lo:lo + bq, :])
        top = jnp.max(scores[0], axis=1, keepdims=True)
        for s in scores[1:]:
            top = jnp.maximum(top, jnp.max(s, axis=1, keepdims=True))
        probs = [jnp.exp2((s - top) * scale2) for s in scores]
        total = jnp.sum(probs[0], axis=1, keepdims=True)
        for p in probs[1:]:
            total = total + jnp.sum(p, axis=1, keepdims=True)
        inv = 1.0 / total
        ctx = None
        for p, vv in zip(probs, vals):
            part = jnp.dot((p * inv).astype(BF16), vv, preferred_element_type=F32)
            ctx = part if ctx is None else ctx + part
        o_ref[lo:lo + bq, :] = ctx.astype(BF16)


def attn_call(qkv, past, n_q, n_kv):
    t = qkv.shape[0]
    group = n_q // n_kv

    def k_spec(arr):
        return pl.BlockSpec((arr.shape[0], HEAD_DIM), lambda h: (0, n_q + h // group))

    def v_spec(arr):
        return pl.BlockSpec((arr.shape[0], HEAD_DIM), lambda h: (0, n_q + n_kv + h // group))

    arrs = list(past) + [qkv]
    seen = sum(p.shape[0] for p in past) * t + t * t // 2
    return pl.pallas_call(
        functools.partial(attn_body, n_past=len(past), bq=256, scale2=HEAD_DIM ** -0.5 * LOG2E),
        out_shape=jax.ShapeDtypeStruct((t, n_q * HEAD_DIM), BF16),
        grid=(n_q,),
        in_specs=[pl.BlockSpec((t, HEAD_DIM), lambda h: (0, h))] + [k_spec(a) for a in arrs] + [v_spec(a) for a in arrs],
        out_specs=pl.BlockSpec((t, HEAD_DIM), lambda h: (0, h)),
        compiler_params=params(),
        cost_estimate=cost(4 * 4 * n_q * seen * HEAD_DIM, 2 * 2 * t * n_q * HEAD_DIM, n_q * seen),
    )(qkv, *arrs, *arrs)


def norm_rows(x, g_row):
    xf = x.astype(F32)
    inv = lax.rsqrt(jnp.mean(xf * xf, axis=-1, keepdims=True) + NORM_EPS)
    return (xf * inv * g_row).astype(BF16)


def first_body(_, x0, x1, x2, x3, g_ref, xp_ref, h_ref):
    x = jnp.concatenate([r[...] for r in (x0, x1, x2, x3)], axis=1)
    xp_ref[...] = x
    h_ref[...] = norm_rows(x, g_ref[...])


def first_call(x, order, g, row0, t):
    d = x.shape[1]
    q = d // 4
    tb = 128
    blk = [pl.BlockSpec((tb, q), lambda r, o, i=i: (row0 // tb + r, o[i])) for i in range(4)]
    row = pl.BlockSpec((tb, d), lambda r, o: (r, 0))
    return pl.pallas_call(
        first_body,
        grid_spec=pltpu.PrefetchScalarGridSpec(
            num_scalar_prefetch=1, grid=(t // tb,),
            in_specs=blk + [pl.BlockSpec((1, d), lambda r, o: (0, 0))], out_specs=[row, row]),
        out_shape=[jax.ShapeDtypeStruct((t, d), BF16)] * 2,
        compiler_params=params(), cost_estimate=cost(10 * t * d, 6 * t * d),
    )(order, x, x, x, x, g)


def add_body(*refs, segs):
    n = len(segs)
    x_ref = refs[0]
    ps, rs = refs[1:1 + n], refs[1 + n:1 + 2 * n]
    g_ref, xo_ref, h_ref = refs[1 + 2 * n:]
    for p, r, seg in zip(ps, rs, segs):
        for src, dst, w in seg:
            a = (p[:, src:src + w].astype(F32) + r[:, src:src + w].astype(F32)).astype(BF16)
            xo_ref[:, dst:dst + w] = (x_ref[:, dst:dst + w].astype(F32) + a.astype(F32)).astype(BF16)
    h_ref[...] = norm_rows(xo_ref[...], g_ref[...])


def add_call(x, units, g):
    t, d = x.shape
    tb = 128
    row = pl.BlockSpec((tb, d), lambda r: (r, 0))
    ps, rs, segs = [u[0] for u in units], [u[1] for u in units], [u[2] for u in units]
    return pl.pallas_call(
        functools.partial(add_body, segs=segs),
        grid=(t // tb,),
        in_specs=[row] + [pl.BlockSpec((tb, a.shape[1]), lambda r: (r, 0)) for a in ps + rs]
        + [pl.BlockSpec((1, d), lambda r: (0, 0))],
        out_specs=[row, row],
        out_shape=[jax.ShapeDtypeStruct((t, d), BF16)] * 2,
        compiler_params=params(), cost_estimate=cost(12 * t * d, 10 * t * d),
    )(x, *ps, *rs, g)


def last_body(_, x_ref, p_ref, r_ref, *rest):
    o_ref = rest[-1]
    a = (p_ref[...].astype(F32) + r_ref[...].astype(F32)).astype(BF16)
    o_ref[...] = (x_ref[...].astype(F32) + a.astype(F32)).astype(BF16)


def last_call(x, unit, order, out_prev, row0, rows):
    p, r, seg = unit
    t, d = x.shape
    w = seg[0][2]
    per = d // 4 // w
    tb = 512
    dst = [s[1] // w for s in seg]
    step = (dst[1] - dst[0]) if len(dst) > 1 else 0
    assert all(dst[j] == dst[0] + j * step for j in range(len(dst)))
    base = dst[0]

    def x_map(j, i, o):
        return (i, base + j * step)

    def o_map(j, i, o):
        pb = base + j * step
        return (row0 // tb + i, o[pb // per] * per + pb % per)

    unit_spec = pl.BlockSpec((tb, w), lambda j, i, o: (i, j))
    args = [x, p, r] + ([out_prev] if out_prev is not None else [])
    return pl.pallas_call(
        last_body,
        grid_spec=pltpu.PrefetchScalarGridSpec(
            num_scalar_prefetch=1, grid=(len(seg), t // tb),
            in_specs=[pl.BlockSpec((tb, w), x_map), unit_spec, unit_spec] + [ANY] * (len(args) - 3),
            out_specs=pl.BlockSpec((tb, w), o_map)),
        out_shape=jax.ShapeDtypeStruct((rows, d), BF16),
        input_output_aliases={4: 0} if out_prev is not None else {},
        compiler_params=params(2), cost_estimate=cost(4 * t * w * len(seg), 8 * t * w * len(seg)),
    )(order, *args)


def solution(mesh):
    n_tp, n_fsdp = mesh.shape["tp"], mesh.shape["fsdp"]
    assert n_tp == 2 and n_fsdp == 4
    tok_spec = P(("dp", "fsdp"), None, None)
    gain_spec = P(None, "fsdp")
    col_spec = P(None, "fsdp", "tp")
    row_spec = P(None, "tp", "fsdp")
    cache_spec = P(None, ("dp", "fsdp"), None, "tp")
    far = [(i, i ^ 2) for i in range(4)]
    near = [(i, i ^ 1) for i in range(4)]
    swap = [(0, 1), (1, 0)]

    def device_fn(x_loc, g_attn, w_q, w_k, w_v, w_o, g_mlp, w_gate, w_up, w_down):
        _, seq, d = x_loc.shape
        n_layers = w_q.shape[0]
        qw, kw = w_q.shape[2], w_k.shape[2]
        f_loc = w_gate.shape[2]
        n_q, n_kv = qw // HEAD_DIM, kw // HEAD_DIM
        quarter = d // 4
        half_t = seq // 2
        assert sum(GU_BLOCKS) * GU_BN == f_loc
        dw = quarter // 2
        me = lax.axis_index("fsdp")
        order = jnp.stack([me, me ^ 1, me ^ 2, me ^ 3]).astype(jnp.int32)
        cos_t, sin_t = rope_tables(seq)
        x2 = x_loc.reshape(seq, d)

        def wide(l, i):
            lo, hi = sum(GU_BLOCKS[:i]) * GU_BN, sum(GU_BLOCKS[:i + 1]) * GU_BN
            return jnp.concatenate([w_gate[l][:, lo:hi], w_up[l][:, lo:hi]], axis=1)

        own = {O: w_o, GATE: w_gate, UP: w_up, DOWN: w_down, G: jnp.concatenate([g_attn, g_mlp], axis=0)}
        for l in range(n_layers):
            own[name_of(O, l)] = w_o[l]
            for i in range(len(GU_BLOCKS)):
                own[name_of(GU, l, i)] = wide(l, i)
            for i in range(2):
                own[name_of(D, l, i)] = w_down[l][:, i * dw:(i + 1) * dw]

        seg_a = [(0, 0, quarter), (quarter, quarter, quarter)]
        seg_own, seg_core = [[(0, 0, dw)], [(0, dw, dw)]], [(0, quarter, quarter)]
        seg_b = [(0, 2 * quarter, quarter), (quarter, 3 * quarter, quarter)]
        seg_d = [[(0, 2 * quarter + i * dw, dw), (dw, 3 * quarter + i * dw, dw)] for i in range(2)]

        xr, cr, nr, part, yr = {}, {}, {}, {}, {}
        hid, hn, qkv, ctx, acts = {}, {}, {}, {}, {}
        out, gains = [None], []

        def pieces(key):
            return [own[key], nr[key], xr[key], cr[key]]

        def kernel(name, dep, op, *idx):
            s, l = idx[-1], idx[-2] if op in (D, QKV, ATTN, OA, OB, ADDO, DA, DB, DC, ADDM) else idx[0]
            if op == FIRST:
                if not gains:
                    rows = jnp.concatenate(pieces(G), axis=1).astype(F32)
                    gains.extend(rows[i:i + 1] for i in range(2 * n_layers))
                hid[s], hn[s] = first_call(dep(x2), order, gains[0], s * half_t, half_t)
                return hn[s]
            if op == QKV:
                rows = slice(s * half_t, (s + 1) * half_t)
                qkv[s] = qkv_call(dep(hn[s]), cos_t[rows], sin_t[rows], pieces(name_of(Q, l)), pieces(name_of(KV, l)),
                                  qw + kw)
                return qkv[s]
            if op == ATTN:
                ctx[s] = attn_call(dep(qkv[s]), [qkv[p] for p in range(s)], n_q, n_kv)
                return ctx[s]
            if op == OA:
                plan = [(0, l, 0), (0, l, dw), (1, l, 0), (1, l, dw)]
                part[name] = cols_call(dep(ctx[s]), [w_o, nr[O]], plan, dw)
                return part[name]
            if op in (DA, DB, DC):
                w = nr[DOWN] if op == DC else w_down
                plan = [(0, l, 0), (0, l, dw)] if op == DC else [(0, l, dw if op == DB else 0)]
                part[name] = cols_call(dep(acts[s]), [w], plan, dw)
                return part[name]
            if op == OB:
                key = name_of(O, l)
                plan = [(0, None, 0), (0, None, dw), (1, None, 0), (1, None, dw)]
                part[name] = cols_call(dep(ctx[s]), [xr[key], cr[key]], plan, dw)
                return part[name]
            if op == D:
                key = name_of(D, l, idx[0])
                part[name] = cols_call(dep(acts[s]), [xr[key], cr[key]], [(0, None, 0), (1, None, 0)], dw)
                return part[name]
            if op == GU:
                i = idx[1]
                key = name_of(GU, l, i)
                acts[s] = gu_call(dep(hn[s]), w_gate, w_up, nr[GATE], nr[UP], xr[key], cr[key],
                                  acts[s] if i else None, sum(GU_BLOCKS[:i]), l, f_loc)
                return acts[s]
            if op == ADDO:
                tags = [name_of(w, l, s) for w in (OA, OB)]
                units = [(part[t], yr[t], g) for t, g in zip(tags, (seg_a, seg_b))]
                hid[s], hn[s] = add_call(dep(hid[s]), units, gains[n_layers + l])
                return hn[s]
            last_l = l if op == ADDM else n_layers - 1
            tags = [name_of(w, last_l, s) for w in (DA, DB, DC)] + [name_of(D, i, last_l, s) for i in range(2)]
            segs = seg_own + [seg_core] + seg_d
            if op == ADDM:
                units = [(part[t], yr[t], g) for t, g in zip(tags, segs)]
                hid[s], hn[s] = add_call(dep(hid[s]), units, gains[l + 1])
                return hn[s]
            i = idx[0]
            unit = (part[tags[i]], yr[tags[i]], segs[i])
            out[0] = last_call(dep(hid[s]), unit, order, out[0], s * half_t, seq)
            return out[0]

        caches = []
        last = None
        for kind, *what in PLAN:
            name = name_of(*what)

            def dep(x):
                return x if last is None else lax.optimization_barrier((x, last))[0]

            if kind == X and what[0] == Q:
                own[name] = dep(w_q)[what[1]]
            elif kind == X and what[0] == KV:
                own[name] = jnp.concatenate([dep(w_k)[what[1]], dep(w_v)[what[1]]], axis=1)
            if kind == X:
                xr[name] = lax.ppermute(dep(own[name]), "fsdp", far)
            elif kind == C:
                cr[name] = lax.ppermute(dep(xr[name]), "fsdp", near)
            elif kind == N:
                nr[name] = lax.ppermute(own[name], "fsdp", near)
            elif kind == Y:
                yr[name] = lax.ppermute(part[name], "tp", swap)
            else:
                last = kernel(name, dep, *what)
            if kind == K and what[0] == QKV and what[-1] == 1:
                caches.append([jnp.concatenate([qkv[s][:, lo:lo + kw] for s in range(2)], axis=0)
                               for lo in (qw, qw + kw)])
        k_all, v_all = (jnp.stack([c[j] for c in caches])[:, None] for j in range(2))
        return out[0].reshape(1, seq, d), k_all, v_all

    return jax.shard_map(
        device_fn, mesh=mesh,
        in_specs=(tok_spec, gain_spec, col_spec, col_spec, col_spec, row_spec, gain_spec, col_spec, col_spec, row_spec),
        out_specs=(tok_spec, cache_spec, cache_spec), check_vma=False)
```
